32 devices in a mesh: tm: 32 (over z, y, x, core).
Axes of the slice: x: 2, y: 2, z: 4, core: 2. Of those that a mesh axis runs over, the one named last changes fastest.
Arguments:
- field: bfloat16 [10752, 2048], P('tm'), may hold values from -52 to 52
- index: float32 [10752, 10], P('tm'), may hold values from -13 to 13
- lag_list: int32 [61], replicated, may hold values from -30 to 30, as said below
- index_offset: int32 [10], replicated, may hold values from 0 to 14, as said below
- sea_mask: int32 [2048], P('tm'), may hold values 0 or 1
Outputs:
- corr_maps: float32 [2048, 10, 61], P('tm')
The draws below stay inside these ranges and needn't reach their ends.
Inputs may be any that keep to these rules, and one draw needn't show every extreme that they name: `lag_list`: each whole number of -30 to 30 appears once. `index_offset`: some index has the extra lead 14.
All inputs are finite; a program needn't handle non-finite values. No bound on the sum of `sea_mask` on one device may be relied on, other than what follows from the above.
Results may differ from the reference program's by a relative error of at most 0.00051.
Values may be sent and summed in bfloat16 or wider, within the bound.
A program may use at most 256 MiB of HBM per device.

```python
import jax
import jax.numpy as jnp
from jax import lax

T_DEV = 336
INDEX_COUNT = 10
MAXLAG = 30
MAXOFF = 14
LAGS = 61
TDAYS = 10752
CELLS = 2048
N_TM = 32


def index_base(key):
    keys = jax.random.split(jax.random.fold_in(key, 11), 2)
    times = jnp.arange(TDAYS, dtype=jnp.float32)[:, None]
    envelope = 1.0 + 2.0 * times / (TDAYS - 1.0)
    noise = jax.random.truncated_normal(keys[0], -4.0, 4.0, (TDAYS, INDEX_COUNT), jnp.float32)
    offset_means = jax.random.uniform(keys[1], (INDEX_COUNT,), jnp.float32, -0.5, 0.5)
    return envelope * noise + offset_means[None, :]


def draw_index(key, part):
    return index_base(key)


def draw_field(key, part):
    series = index_base(key)
    keys = jax.random.split(jax.random.fold_in(key, 23), 6)
    linked = jax.random.randint(keys[0], (CELLS,), 0, INDEX_COUNT)
    delays = jax.random.randint(keys[1], (CELLS,), -MAXLAG, MAXLAG + MAXOFF + 1)
    weights = jax.random.uniform(keys[2], (CELLS,), jnp.float32, 0.3, 1.0) * jnp.where(jax.random.randint(keys[3], (CELLS,), 0, 2) == 0, -1.0, 1.0)
    scales = jnp.exp(jax.random.uniform(keys[4], (CELLS,), jnp.float32, jnp.log(0.3), jnp.log(3.0)))
    times = jnp.arange(TDAYS, dtype=jnp.int32)[:, None]
    source = jnp.clip(times - delays[None, :], 0, TDAYS - 1)
    signal = series[source, linked[None, :]]
    noise = jax.random.truncated_normal(keys[5], -4.0, 4.0, (TDAYS, CELLS), jnp.float32)
    cell_means = 0.5 * weights
    return (scales[None, :] * (weights[None, :] * signal + noise + cell_means[None, :])).astype(jnp.bfloat16)


def draw_lag_list(key, part):
    order = jax.random.permutation(jax.random.fold_in(key, 31), LAGS)
    return (order - MAXLAG).astype(jnp.int32)


def draw_index_offset(key, part):
    keys = jax.random.split(jax.random.fold_in(key, 37), 2)
    series_values = jax.random.randint(keys[0], (INDEX_COUNT,), 0, MAXOFF + 1)
    chosen = jax.random.randint(keys[1], (), 0, INDEX_COUNT)
    return series_values.at[chosen].set(MAXOFF).astype(jnp.int32)


def place_ends(drawn, stream_key, smallest, high):
    dims = drawn.shape
    index_at = [jax.random.randint(jax.random.fold_in(stream_key, axis), (), 0, dims[axis]) for axis in range(len(dims))]
    drawn = drawn.at[tuple(index_at)].set(smallest)
    longest = dims.index(max(dims))
    index_at[longest] = (index_at[longest] + 1) % dims[longest]
    return drawn.at[tuple(index_at)].set(high)


def setup_inputs(seed: int = 0) -> dict:
    streams_of = jax.random.split(jax.random.key(seed), 6)
    field = draw_field(jax.random.fold_in(streams_of[5], 71), 0)
    index = draw_index(jax.random.fold_in(streams_of[5], 71), 0)
    lag_list = draw_lag_list(jax.random.fold_in(streams_of[5], 71), 0)
    index_offset = draw_index_offset(jax.random.fold_in(streams_of[5], 71), 0)
    sea_mask = place_ends((jax.random.randint(streams_of[4], (CELLS,), 0, 10) < 7).astype(jnp.int32), jax.random.fold_in(streams_of[4], 1), 0, 1)
    return dict(field=field, index=index, lag_list=lag_list, index_offset=index_offset, sea_mask=sea_mask)


def build_window_sums(padded, begin, length, reach, lag_low):
    count = reach + lag_low + 1
    piece = lax.dynamic_slice_in_dim(padded, begin, length + reach + lag_low, 0)
    windows = jnp.stack([piece[reach + lag_low - j:reach + lag_low - j + length] for j in range(count)], 1)
    return windows.reshape(length, count * padded.shape[1])

def lag_selector(shifts, reach, lag_low):
    count = reach + lag_low + 1
    places = jnp.arange(count, dtype=jnp.int32)
    return (places[None, :, None] == (shifts + lag_low)[:, None, :]).astype(jnp.float32)

def pick_lags(accum, selector):
    kcount, count, lcount = selector.shape
    spread = accum.reshape(accum.shape[0], count, kcount)
    chosen = jnp.einsum('cjk,kjl->ckl', spread, selector, precision=lax.Precision.HIGHEST)
    return chosen.reshape(accum.shape[0], kcount * lcount)

def reference(field, index, lag_list, index_offset, sea_mask):
    reach = MAXLAG + MAXOFF
    count = reach + MAXLAG + 1
    total_days = TDAYS * 1.0
    mean_i = lax.optimization_barrier(jnp.sum(index, 0)) / total_days
    var_i = lax.optimization_barrier(jnp.sum(index * index, 0)) / total_days - mean_i * mean_i
    centered = (index - mean_i).astype(jnp.bfloat16)
    shifts = (lag_list[None, :] + index_offset[:, None]).astype(jnp.int32)
    padded = jnp.pad(centered, ((reach, reach), (0, 0)))
    running_total = jnp.concatenate([jnp.zeros((1, INDEX_COUNT), jnp.float32), jnp.cumsum(padded.astype(jnp.float32), 0)], 0)
    upper_bound = (TDAYS - shifts + reach).astype(jnp.int32)
    lower_bound = (reach - shifts).astype(jnp.int32)
    series_number = jnp.arange(INDEX_COUNT, dtype=jnp.int32)[:, None]
    prefix_totals = running_total[upper_bound, series_number] - running_total[lower_bound, series_number]
    selector = lag_selector(shifts, reach, MAXLAG)
    block_rows = 8 * T_DEV
    turns = N_TM // 8

    def one_block(carry, turn):
        accum, first_sum, second_sum = carry
        begin = (turn * block_rows).astype(jnp.int32)
        rows = lax.dynamic_slice_in_dim(field, begin, block_rows, 0)
        windows = build_window_sums(padded, begin, block_rows, reach, MAXLAG)
        accum = accum + lax.dot_general(rows, windows, (((0,), (0,)), ((), ())), preferred_element_type=jnp.float32)
        wide = rows.astype(jnp.float32)
        return ((accum, first_sum + lax.optimization_barrier(jnp.sum(wide, 0)), second_sum + lax.optimization_barrier(jnp.sum(wide * wide, 0))), None)
    start_carry = (jnp.zeros((CELLS, count * INDEX_COUNT), jnp.float32), jnp.zeros((CELLS,), jnp.float32), jnp.zeros((CELLS,), jnp.float32))
    (accum, first_sum, second_sum), unused = lax.scan(one_block, start_carry, jnp.arange(turns, dtype=jnp.int32))
    products = pick_lags(accum, selector)
    mean_x = first_sum / total_days
    var_x = second_sum / total_days - mean_x * mean_x
    numer = products.reshape(CELLS, INDEX_COUNT, LAGS) - mean_x[:, None, None] * prefix_totals[None]
    scale = total_days * jnp.sqrt(var_x + 1e-06)[:, None, None] * jnp.sqrt(var_i + 1e-06)[None, :, None]
    return numer / scale * sea_mask.astype(jnp.float32)[:, None, None]
```

```python
import functools

import jax
import jax.numpy as jnp
from jax import lax
from jax.experimental import pallas as pl
from jax.experimental.pallas import tpu as pltpu
from jax.sharding import PartitionSpec as P

MAXLAG = 30
MAXOFF = 14
PLACES = 2 * MAXLAG + MAXOFF + 1
MESH = pl.DeviceIdType.MESH


def round_up(value, unit):
    return -(-value // unit) * unit


def kernel(
    sizes,
    field_ref,
    idx_ref,
    acc_out,
    stat_out,
    tot_out,
    var_out,
    recv,
    idx_all,
    win,
    acc,
    acc_in,
    field_send,
    field_recv,
    one_send,
    one_recv,
    two_send,
    two_recv,
    last_send,
    last_recv,
    own_sem,
):
    devices, t_dev, kcount, kpad, rows, low = sizes
    chips = devices // 2
    high = chips // low
    lanes = idx_ref.shape[1]
    wide = lanes + 128
    me = lax.axis_index("tm")
    chip = lax.div(me, 2)
    core = lax.rem(me, 2)
    hi = lax.div(chip, low)
    lo = lax.rem(chip, low)
    partner = chip * 2 + (1 - core)
    cells = recv.shape[2]

    def slot_of(device):
        at = lax.div(device, 2)
        return (lax.rem(device, 2) * low + lax.rem(at, low)) * high + lax.div(at, low)

    def block(at):
        return field_ref.at[:, pl.ds(pl.multiple_of(at * cells, cells), cells)]

    my_slot = slot_of(me)

    def one_copy(step):
        to = lax.rem(hi + step, high)
        return pltpu.make_async_remote_copy(
            src_ref=idx_ref,
            dst_ref=idx_all.at[my_slot],
            send_sem=one_send.at[step],
            recv_sem=one_recv.at[step],
            device_id=((to * low + lo) * 2 + core,),
            device_id_type=MESH,
        )

    def two_copy(step):
        to = lax.rem(lo + step, low)
        part = idx_all.at[pl.ds((core * low + lo) * high, high)]
        return pltpu.make_async_remote_copy(
            src_ref=part,
            dst_ref=part,
            send_sem=two_send.at[step],
            recv_sem=two_recv.at[step],
            device_id=((hi * low + to) * 2 + core,),
            device_id_type=MESH,
        )

    def last_copy():
        part = idx_all.at[pl.ds(core * chips, chips)]
        return pltpu.make_async_remote_copy(
            src_ref=part,
            dst_ref=part,
            send_sem=last_send.at[0],
            recv_sem=last_recv.at[0],
            device_id=(partner,),
            device_id_type=MESH,
        )

    def field_copy(step):
        to = lax.rem(chip + step, chips)
        return pltpu.make_async_remote_copy(
            src_ref=block(to),
            dst_ref=recv.at[step],
            send_sem=field_send.at[step],
            recv_sem=field_recv.at[step],
            device_id=(to * 2 + core,),
            device_id_type=MESH,
        )

    def each(low_step, high_step, act):
        def body(step, carry):
            act(step)
            return carry

        lax.fori_loop(low_step, high_step, body, 0)

    own_idx = pltpu.make_async_copy(idx_ref, idx_all.at[my_slot], own_sem.at[0])
    own_field = pltpu.make_async_copy(block(chip), recv.at[0], own_sem.at[1])
    own_idx.start()
    own_field.start()
    each(1, high, lambda s: one_copy(s).start())
    each(1, chips, lambda s: field_copy(s).start())
    own_idx.wait()
    own_field.wait()
    each(1, high, lambda s: one_copy(s).wait())
    each(1, low, lambda s: two_copy(s).start())
    each(1, low, lambda s: two_copy(s).wait())
    last_copy().start()
    last_copy().wait()

    total_days = devices * t_dev * 1.0

    def sum_body(at, carry):
        first, second = carry
        value = idx_all[at]
        return first + value, second + value * value

    zero = jnp.zeros((kpad, lanes), jnp.float32)
    first, second = lax.fori_loop(0, devices, sum_body, (zero, zero))
    mean = jnp.sum(first, 1, keepdims=True) / total_days
    var = jnp.sum(second, 1, keepdims=True) / total_days - mean * mean
    var_out[...] = jnp.broadcast_to(var, (kpad, 128))
    valid = lax.broadcasted_iota(jnp.int32, (kpad, lanes), 1) < t_dev

    def center_body(at, carry):
        value = (idx_all[at] - mean).astype(jnp.bfloat16).astype(jnp.float32)
        value = jnp.where(valid, value, 0.0)
        idx_all[at] = value
        return carry + value

    centered_sum = jnp.sum(lax.fori_loop(0, devices, center_body, zero), 1, keepdims=True)
    day = lax.broadcasted_iota(jnp.int32, (lanes, 128), 0)
    shift = lax.broadcasted_iota(jnp.int32, (lanes, 128), 1) - MAXLAG
    late = jnp.where((day >= t_dev - shift) & (day < t_dev), 1.0, 0.0).astype(jnp.bfloat16)
    early = jnp.where(day < -shift, 1.0, 0.0).astype(jnp.bfloat16)
    dropped = jnp.dot(
        idx_all[slot_of(devices - 1)].astype(jnp.bfloat16),
        late,
        preferred_element_type=jnp.float32,
    ) + jnp.dot(
        idx_all[0].astype(jnp.bfloat16), early, preferred_element_type=jnp.float32
    )
    tot_out[...] = centered_sum - dropped

    acc[...] = jnp.zeros_like(acc)
    place = lax.broadcasted_iota(jnp.int32, (kpad, wide), 1)
    tail = jnp.zeros((kpad, 128), jnp.float32)
    reach = 64

    def source_body(step, carry):
        from_chip = lax.rem(chip - step + chips, chips)
        device = from_chip * 2 + core
        before = idx_all[slot_of(jnp.maximum(device - 1, 0))]
        after = idx_all[slot_of(jnp.minimum(device + 1, devices - 1))]
        before = before * jnp.where(device > 0, 1.0, 0.0)
        after = after * jnp.where(device < devices - 1, 1.0, 0.0)
        here = jnp.concatenate([idx_all[slot_of(device)], tail], 1)
        before = jnp.concatenate([before, tail], 1)
        after = jnp.concatenate([after, tail], 1)
        left = pltpu.roll(before, (reach - t_dev) % wide, 1)
        mid = pltpu.roll(here, reach, 1)
        right = pltpu.roll(after, reach + t_dev, 1)
        ext = jnp.where(place < reach, left, jnp.where(place < reach + t_dev, mid, right))
        for k in range(kcount):
            line = jnp.broadcast_to(ext[k : k + 1], (rows, wide))
            turned = pltpu.roll(line, wide - reach - MAXLAG, 1, stride=1, stride_axis=0)
            win[k * rows : (k + 1) * rows, :] = turned[:, :lanes].astype(jnp.bfloat16)

        @pl.when(step > 0)
        def _():
            field_copy(step).wait()

        got = recv[step]
        acc[0 : kcount * rows, :] += jnp.dot(
            win[:, :t_dev], got, preferred_element_type=jnp.float32
        )
        value = got.astype(jnp.float32)
        acc[kcount * rows : kcount * rows + 1, :] += jnp.sum(value, 0, keepdims=True)
        acc[kcount * rows + 1 : kcount * rows + 2, :] += jnp.sum(value * value, 0, keepdims=True)
        return carry

    lax.fori_loop(0, chips, source_body, 0)
    swap = pltpu.make_async_remote_copy(
        src_ref=acc,
        dst_ref=acc_in,
        send_sem=last_send.at[1],
        recv_sem=last_recv.at[1],
        device_id=(partner,),
        device_id_type=MESH,
    )
    swap.start()
    swap.wait()
    count = kcount * rows
    acc_out[...] = acc[0:count, :] + acc_in[0:count, :]
    stat_out[...] = acc[count:, :] + acc_in[count:, :]


def gather_products(field, index_rows, devices, kcount):
    t_dev, cells_all = field.shape
    kpad, lanes = index_rows.shape
    chips = devices // 2
    cells = cells_all // chips
    rows = round_up(PLACES, 16)
    low = 1
    while low * low < chips:
        low *= 2
    high = chips // low
    sizes = (devices, t_dev, kcount, kpad, rows, low)
    dma = pltpu.SemaphoreType.DMA
    f32 = jnp.float32
    return pl.pallas_call(
        functools.partial(kernel, sizes),
        out_shape=(
            jax.ShapeDtypeStruct((kcount * rows, cells), f32),
            jax.ShapeDtypeStruct((8, cells), f32),
            jax.ShapeDtypeStruct((kpad, 128), f32),
            jax.ShapeDtypeStruct((kpad, 128), f32),
        ),
        in_specs=[pl.BlockSpec(memory_space=pltpu.VMEM)] * 2,
        out_specs=(pl.BlockSpec(memory_space=pltpu.VMEM),) * 4,
        scratch_shapes=[
            pltpu.VMEM((chips, t_dev, cells), jnp.bfloat16),
            pltpu.VMEM((devices, kpad, lanes), f32),
            pltpu.VMEM((kcount * rows, lanes), jnp.bfloat16),
            pltpu.VMEM((kcount * rows + 8, cells), f32),
            pltpu.VMEM((kcount * rows + 8, cells), f32),
            dma((chips,)),
            dma((chips,)),
            dma((high,)),
            dma((high,)),
            dma((low,)),
            dma((low,)),
            dma((2,)),
            dma((2,)),
            dma((2,)),
        ],
        compiler_params=pltpu.CompilerParams(
            has_side_effects=True, vmem_limit_bytes=56 * 1024 * 1024
        ),
    )(field, index_rows)


def shards(field, index, lag_list, index_offset, sea_mask):
    t_dev = field.shape[0]
    devices = lax.axis_size("tm")
    total_days = t_dev * devices * 1.0
    kcount = index.shape[1]
    cell_count = sea_mask.shape[0]
    kpad = round_up(kcount, 16)
    lanes = round_up(t_dev, 128)
    rows = round_up(PLACES, 16)
    index_rows = jnp.pad(index.T, ((0, kpad - kcount), (0, lanes - t_dev)))
    products, stats, totals, var_i = gather_products(field, index_rows, devices, kcount)
    begin = lax.rem(lax.axis_index("tm"), 2) * cell_count
    products = lax.dynamic_slice_in_dim(products, begin, cell_count, 1)
    stats = lax.dynamic_slice_in_dim(stats, begin, cell_count, 1)
    shifts = lag_list[None, :] + index_offset[:, None]
    places = jnp.arange(rows, dtype=jnp.int32)
    selector = (places[None, :, None] == (shifts + MAXLAG)[:, None, :]).astype(jnp.float32)
    mean_x = stats[0] / total_days
    var_x = stats[1] / total_days - mean_x * mean_x
    spread = products.reshape(kcount, rows, cell_count)
    spread = spread - mean_x[None, None, :] * totals[:kcount, :rows, None]
    inner = jnp.sqrt(var_x + 1e-06)[None, None, :]
    outer = jnp.sqrt(var_i[:kcount, 0] + 1e-06)[:, None, None]
    spread = spread / (total_days * inner * outer)
    spread = spread * sea_mask.astype(jnp.float32)[None, None, :]
    return jnp.einsum("kjc,kjl->ckl", spread, selector, precision=lax.Precision.HIGHEST)


def solution(mesh):
    return jax.shard_map(
        shards,
        mesh=mesh,
        in_specs=(P("tm", None), P("tm", None), P(), P(), P("tm")),
        out_specs=P("tm", None, None),
        check_vma=False,
    )
```

```python
import functools

import jax
import jax.numpy as jnp
from jax import lax
from jax.experimental import pallas as pl
from jax.experimental.pallas import tpu as pltpu
from jax.sharding import PartitionSpec as P

MAXLAG = 30
MAXOFF = 14
PLACES = 2 * MAXLAG + MAXOFF + 1
MESH = pl.DeviceIdType.MESH


def round_up(value, unit):
    return -(-value // unit) * unit


def kernel(
    sizes,
    field_hbm,
    index_ref,
    lag_ref,
    offset_ref,
    mask_ref,
    out_ref,
    field_ref,
    idx_ref,
    recv,
    idx_all,
    win,
    acc,
    acc_in,
    field_send,
    field_recv,
    one_send,
    one_recv,
    two_send,
    two_recv,
    last_send,
    last_recv,
    own_sem,
):
    devices, t_dev, kcount, kpad, rows, low = sizes
    chips = devices // 2
    high = chips // low
    lanes = idx_ref.shape[1]
    wide = lanes + 128
    me = lax.axis_index("tm")
    chip = lax.div(me, 2)
    core = lax.rem(me, 2)
    hi = lax.div(chip, low)
    lo = lax.rem(chip, low)
    partner = chip * 2 + (1 - core)
    cells = recv.shape[2]

    def across(step):
        other, bit = 0, 1
        while bit < chips:
            flip = lax.rem(lax.div(chip, bit) + lax.div(step, bit), 2)
            other, bit = other + flip * bit, bit * 2
        return other

    def slot_of(device):
        at = lax.div(device, 2)
        return (lax.rem(device, 2) * low + lax.rem(at, low)) * high + lax.div(at, low)

    def block(at):
        return field_ref.at[:, pl.ds(pl.multiple_of(at * cells, cells), cells)]

    my_slot = slot_of(me)

    def one_copy(step):
        to = lax.rem(hi + step, high)
        return pltpu.make_async_remote_copy(
            src_ref=idx_ref,
            dst_ref=idx_all.at[my_slot],
            send_sem=one_send.at[step],
            recv_sem=one_recv.at[step],
            device_id=((to * low + lo) * 2 + core,),
            device_id_type=MESH,
        )

    def two_copy(step):
        to = lax.rem(lo + step, low)
        part = idx_all.at[pl.ds((core * low + lo) * high, high)]
        return pltpu.make_async_remote_copy(
            src_ref=part,
            dst_ref=part,
            send_sem=two_send.at[step],
            recv_sem=two_recv.at[step],
            device_id=((hi * low + to) * 2 + core,),
            device_id_type=MESH,
        )

    def last_copy():
        part = idx_all.at[pl.ds(core * chips, chips)]
        return pltpu.make_async_remote_copy(
            src_ref=part,
            dst_ref=part,
            send_sem=last_send.at[0],
            recv_sem=last_recv.at[0],
            device_id=(partner,),
            device_id_type=MESH,
        )

    def field_copy(step):
        to = across(step)
        return pltpu.make_async_remote_copy(
            src_ref=block(to),
            dst_ref=recv.at[step],
            send_sem=field_send.at[step],
            recv_sem=field_recv.at[step],
            device_id=(to * 2 + core,),
            device_id_type=MESH,
        )

    def each(low_step, high_step, act):
        def body(step, carry):
            act(step)
            return carry

        lax.fori_loop(low_step, high_step, body, 0)

    load = pltpu.make_async_copy(field_hbm, field_ref, own_sem.at[2])
    load.start()
    barrier = pltpu.get_barrier_semaphore()

    def greet(device):
        pl.semaphore_signal(barrier, inc=1, device_id=(device,), device_id_type=MESH)

    each(1, chips, lambda s: greet(across(s) * 2 + core))
    greet(partner)
    idx_ref[...] = jnp.zeros_like(idx_ref)
    idx_ref[0:kcount, 0:t_dev] = index_ref[...]
    acc[...] = jnp.zeros_like(acc)
    pl.semaphore_wait(barrier, chips)
    load.wait()
    own_idx = pltpu.make_async_copy(idx_ref, idx_all.at[my_slot], own_sem.at[0])
    own_field = pltpu.make_async_copy(block(chip), recv.at[0], own_sem.at[1])
    own_idx.start()
    own_field.start()
    each(1, high, lambda s: one_copy(s).start())
    each(1, chips, lambda s: field_copy(s).start())
    own_idx.wait()
    own_field.wait()
    each(1, high, lambda s: one_copy(s).wait())
    each(1, low, lambda s: two_copy(s).start())
    each(1, low, lambda s: two_copy(s).wait())
    last_copy().start()
    last_copy().wait()

    total_days = devices * t_dev * 1.0

    def sum_body(at, carry):
        first, second = carry
        value = idx_all[at]
        return first + value, second + value * value

    zero = jnp.zeros((kpad, lanes), jnp.float32)
    first, second = lax.fori_loop(0, devices, sum_body, (zero, zero))
    mean = jnp.sum(first, 1, keepdims=True) / total_days
    var = jnp.sum(second, 1, keepdims=True) / total_days - mean * mean
    valid = lax.broadcasted_iota(jnp.int32, (kpad, lanes), 1) < t_dev

    def center_body(at, carry):
        value = (idx_all[at] - mean).astype(jnp.bfloat16).astype(jnp.float32)
        value = jnp.where(valid, value, 0.0)
        idx_all[at] = value
        return carry + value

    centered_sum = jnp.sum(lax.fori_loop(0, devices, center_body, zero), 1, keepdims=True)
    day = lax.broadcasted_iota(jnp.int32, (lanes, 128), 0)
    shift = lax.broadcasted_iota(jnp.int32, (lanes, 128), 1) - MAXLAG
    late = jnp.where((day >= t_dev - shift) & (day < t_dev), 1.0, 0.0).astype(jnp.bfloat16)
    early = jnp.where(day < -shift, 1.0, 0.0).astype(jnp.bfloat16)
    dropped = jnp.dot(
        idx_all[slot_of(devices - 1)].astype(jnp.bfloat16),
        late,
        preferred_element_type=jnp.float32,
    ) + jnp.dot(
        idx_all[0].astype(jnp.bfloat16), early, preferred_element_type=jnp.float32
    )
    totals = jnp.transpose(centered_sum - dropped)

    place = lax.broadcasted_iota(jnp.int32, (kpad, wide), 1)
    tail = jnp.zeros((kpad, 128), jnp.float32)
    reach = 64

    def window_body(step, carry):
        device = across(step) * 2 + core
        before = idx_all[slot_of(jnp.maximum(device - 1, 0))]
        after = idx_all[slot_of(jnp.minimum(device + 1, devices - 1))]
        before = before * jnp.where(device > 0, 1.0, 0.0)
        after = after * jnp.where(device < devices - 1, 1.0, 0.0)
        here = jnp.concatenate([idx_all[slot_of(device)], tail], 1)
        before = jnp.concatenate([before, tail], 1)
        after = jnp.concatenate([after, tail], 1)
        left = pltpu.roll(before, (reach - t_dev) % wide, 1)
        mid = pltpu.roll(here, reach, 1)
        right = pltpu.roll(after, reach + t_dev, 1)
        ext = jnp.where(place < reach, left, jnp.where(place < reach + t_dev, mid, right))
        for k in range(kcount):
            line = jnp.broadcast_to(ext[k : k + 1], (rows, wide))
            turned = pltpu.roll(line, wide - reach - MAXLAG, 1, stride=1, stride_axis=0)
            win[step, k * rows : (k + 1) * rows, :] = turned[:, :lanes].astype(jnp.bfloat16)
        return carry

    def source_body(step, carry):
        @pl.when(step > 0)
        def _():
            field_copy(step).wait()

        got = recv[step]
        acc[0 : kcount * rows, :] += jnp.dot(
            win[step, :, :t_dev], got, preferred_element_type=jnp.float32
        )
        value = got.astype(jnp.float32)
        acc[kcount * rows : kcount * rows + 1, :] += jnp.sum(value, 0, keepdims=True)
        acc[kcount * rows + 1 : kcount * rows + 2, :] += jnp.sum(value * value, 0, keepdims=True)
        return carry

    lax.fori_loop(0, chips, window_body, 0)
    lax.fori_loop(0, chips, source_body, 0)
    swap = pltpu.make_async_remote_copy(
        src_ref=acc,
        dst_ref=acc_in,
        send_sem=last_send.at[1],
        recv_sem=last_recv.at[1],
        device_id=(partner,),
        device_id_type=MESH,
    )
    swap.start()
    swap.wait()
    count = kcount * rows
    half = cells // 2

    def mine(begin, end):
        total = acc[begin:end, :] + acc_in[begin:end, :]
        return jnp.where(core == 0, total[:, :half], total[:, half:])

    mean_x = mine(count, count + 1) / total_days
    var_x = mine(count + 1, count + 2) / total_days - mean_x * mean_x
    inner = total_days * jnp.sqrt(var_x + 1e-06)
    mask = mask_ref[...].astype(jnp.float32)
    outer = jnp.sqrt(var + 1e-06)
    lag = lag_ref[...]
    row = lax.broadcasted_iota(jnp.int32, (rows, lag.shape[1]), 0)
    for k in range(kcount):
        numer = mine(k * rows, (k + 1) * rows) - mean_x * totals[0:rows, k : k + 1]
        value = numer / (inner * outer[k : k + 1]) * mask
        chosen = jnp.where(row == lag + (offset_ref[k] + MAXLAG), 1.0, 0.0)
        out_ref[k] = lax.dot_general(
            value,
            chosen,
            (((0,), (0,)), ((), ())),
            precision=lax.Precision.HIGHEST,
            preferred_element_type=jnp.float32,
        )


def shards(field, index, lag_list, index_offset, sea_mask):
    t_dev, cells_all = field.shape
    devices = lax.axis_size("tm")
    kcount = index.shape[1]
    kpad = round_up(kcount, 16)
    lanes = round_up(t_dev, 128)
    rows = round_up(PLACES, 16)
    chips = devices // 2
    cells = cells_all // chips
    low = 1
    while low * low < chips:
        low *= 2
    high = chips // low
    sizes = (devices, t_dev, kcount, kpad, rows, low)
    dma = pltpu.SemaphoreType.DMA
    f32 = jnp.float32
    vmem = pl.BlockSpec(memory_space=pltpu.VMEM)
    maps = pl.pallas_call(
        functools.partial(kernel, sizes),
        out_shape=jax.ShapeDtypeStruct((kcount, cells // 2, lag_list.shape[0]), f32),
        in_specs=[
            pl.BlockSpec(memory_space=pl.ANY),
            vmem,
            vmem,
            pl.BlockSpec(memory_space=pltpu.SMEM),
            vmem,
        ],
        out_specs=vmem,
        scratch_shapes=[
            pltpu.VMEM((t_dev, cells_all), jnp.bfloat16),
            pltpu.VMEM((kpad, lanes), f32),
            pltpu.VMEM((chips, t_dev, cells), jnp.bfloat16),
            pltpu.VMEM((devices, kpad, lanes), f32),
            pltpu.VMEM((chips, kcount * rows, lanes), jnp.bfloat16),
            pltpu.VMEM((kcount * rows + 8, cells), f32),
            pltpu.VMEM((kcount * rows + 8, cells), f32),
            dma((chips,)),
            dma((chips,)),
            dma((high,)),
            dma((high,)),
            dma((low,)),
            dma((low,)),
            dma((2,)),
            dma((2,)),
            dma((3,)),
        ],
        compiler_params=pltpu.CompilerParams(
            collective_id=0, has_side_effects=True, vmem_limit_bytes=60 * 1024 * 1024
        ),
    )(field, index.T, lag_list[None, :], index_offset, sea_mask[None, :])
    return jnp.transpose(maps, (1, 0, 2))


def solution(mesh):
    return jax.shard_map(
        shards,
        mesh=mesh,
        in_specs=(P("tm", None), P("tm", None), P(), P(), P("tm")),
        out_specs=P("tm", None, None),
        check_vma=False,
    )
```

```python
import functools

import jax
import jax.numpy as jnp
from jax import lax
from jax.experimental import pallas as pl
from jax.experimental.pallas import tpu as pltpu
from jax.sharding import PartitionSpec as P

MAXLAG = 30
MAXOFF = 14
PLACES = 2 * MAXLAG + MAXOFF + 1
MESH = pl.DeviceIdType.MESH


def round_up(value, unit):
    return -(-value // unit) * unit


def kernel(
    sizes,
    field_hbm,
    index_ref,
    lag_ref,
    offset_ref,
    mask_ref,
    out_ref,
    field_ref,
    idx_ref,
    recv,
    idx_all,
    win,
    acc,
    acc_in,
    field_send,
    field_recv,
    one_send,
    one_recv,
    two_send,
    two_recv,
    last_send,
    last_recv,
    own_sem,
):
    devices, t_dev, kcount, kpad, rows, low = sizes
    chips = devices // 2
    high = chips // low
    lanes = idx_ref.shape[1]
    wide = lanes + 128
    me = lax.axis_index("tm")
    chip = lax.div(me, 2)
    core = lax.rem(me, 2)
    hi = lax.div(chip, low)
    lo = lax.rem(chip, low)
    partner = chip * 2 + (1 - core)
    cells = recv.shape[2]

    def across(step):
        other, bit = 0, 1
        while bit < chips:
            flip = lax.rem(lax.div(chip, bit) + lax.div(step, bit), 2)
            other, bit = other + flip * bit, bit * 2
        return other

    def slot_of(device):
        at = lax.div(device, 2)
        return (lax.rem(device, 2) * low + lax.rem(at, low)) * high + lax.div(at, low)

    def block(at):
        return field_ref.at[:, pl.ds(pl.multiple_of(at * cells, cells), cells)]

    my_slot = slot_of(me)

    def one_copy(step):
        to = lax.rem(hi + step, high)
        return pltpu.make_async_remote_copy(
            src_ref=idx_ref,
            dst_ref=idx_all.at[my_slot],
            send_sem=one_send.at[step],
            recv_sem=one_recv.at[step],
            device_id=((to * low + lo) * 2 + core,),
            device_id_type=MESH,
        )

    def two_copy(step):
        to = lax.rem(lo + step, low)
        part = idx_all.at[pl.ds((core * low + lo) * high, high)]
        return pltpu.make_async_remote_copy(
            src_ref=part,
            dst_ref=part,
            send_sem=two_send.at[step],
            recv_sem=two_recv.at[step],
            device_id=((hi * low + to) * 2 + core,),
            device_id_type=MESH,
        )

    def last_copy():
        part = idx_all.at[pl.ds(core * chips, chips)]
        return pltpu.make_async_remote_copy(
            src_ref=part,
            dst_ref=part,
            send_sem=last_send.at[0],
            recv_sem=last_recv.at[0],
            device_id=(partner,),
            device_id_type=MESH,
        )

    def field_copy(step):
        to = across(step)
        return pltpu.make_async_remote_copy(
            src_ref=block(to),
            dst_ref=recv.at[step],
            send_sem=field_send.at[step],
            recv_sem=field_recv.at[step],
            device_id=(to * 2 + core,),
            device_id_type=MESH,
        )

    def each(low_step, high_step, act):
        def body(step, carry):
            act(step)
            return carry

        lax.fori_loop(low_step, high_step, body, 0)

    load = pltpu.make_async_copy(field_hbm, field_ref, own_sem.at[2])
    load.start()
    barrier = pltpu.get_barrier_semaphore()

    def greet(device):
        pl.semaphore_signal(barrier, inc=1, device_id=(device,), device_id_type=MESH)

    each(1, chips, lambda s: greet(across(s) * 2 + core))
    greet(partner)
    idx_ref[...] = jnp.zeros_like(idx_ref)
    idx_ref[0:kcount, 0:t_dev] = index_ref[...]
    acc[...] = jnp.zeros_like(acc)
    pl.semaphore_wait(barrier, chips)
    load.wait()
    own_idx = pltpu.make_async_copy(idx_ref, idx_all.at[my_slot], own_sem.at[0])
    own_field = pltpu.make_async_copy(block(chip), recv.at[0], own_sem.at[1])
    own_idx.start()
    own_field.start()
    each(1, high, lambda s: one_copy(s).start())
    each(1, chips, lambda s: field_copy(s).start())
    own_idx.wait()
    own_field.wait()
    each(1, high, lambda s: one_copy(s).wait())
    each(1, low, lambda s: two_copy(s).start())
    each(1, low, lambda s: two_copy(s).wait())
    last_copy().start()
    last_copy().wait()

    total_days = devices * t_dev * 1.0

    def sum_body(at, carry):
        first, second = carry
        value = idx_all[at]
        return first + value, second + value * value

    zero = jnp.zeros((kpad, lanes), jnp.float32)
    first, second = lax.fori_loop(0, devices, sum_body, (zero, zero))
    mean = jnp.sum(first, 1, keepdims=True) / total_days
    var = jnp.sum(second, 1, keepdims=True) / total_days - mean * mean
    valid = lax.broadcasted_iota(jnp.int32, (kpad, lanes), 1) < t_dev

    def center_body(at, carry):
        value = (idx_all[at] - mean).astype(jnp.bfloat16).astype(jnp.float32)
        value = jnp.where(valid, value, 0.0)
        idx_all[at] = value
        return carry + value

    centered_sum = jnp.sum(lax.fori_loop(0, devices, center_body, zero), 1, keepdims=True)
    day = lax.broadcasted_iota(jnp.int32, (lanes, 128), 0)
    shift = lax.broadcasted_iota(jnp.int32, (lanes, 128), 1) - MAXLAG
    late = jnp.where((day >= t_dev - shift) & (day < t_dev), 1.0, 0.0).astype(jnp.bfloat16)
    early = jnp.where(day < -shift, 1.0, 0.0).astype(jnp.bfloat16)
    dropped = jnp.dot(
        idx_all[slot_of(devices - 1)].astype(jnp.bfloat16),
        late,
        preferred_element_type=jnp.float32,
    ) + jnp.dot(
        idx_all[0].astype(jnp.bfloat16), early, preferred_element_type=jnp.float32
    )
    fill = jnp.zeros((round_up(kpad, 8) - kpad, 128), jnp.float32)
    totals = jnp.transpose(jnp.concatenate([centered_sum - dropped, fill], 0))

    place = lax.broadcasted_iota(jnp.int32, (kpad, wide), 1)
    tail = jnp.zeros((kpad, 128), jnp.float32)
    reach = 64

    def window_body(step, carry):
        device = across(step) * 2 + core
        before = idx_all[slot_of(jnp.maximum(device - 1, 0))]
        after = idx_all[slot_of(jnp.minimum(device + 1, devices - 1))]
        before = before * jnp.where(device > 0, 1.0, 0.0)
        after = after * jnp.where(device < devices - 1, 1.0, 0.0)
        here = jnp.concatenate([idx_all[slot_of(device)], tail], 1)
        before = jnp.concatenate([before, tail], 1)
        after = jnp.concatenate([after, tail], 1)
        left = pltpu.roll(before, (reach - t_dev) % wide, 1)
        mid = pltpu.roll(here, reach, 1)
        right = pltpu.roll(after, reach + t_dev, 1)
        ext = jnp.where(place < reach, left, jnp.where(place < reach + t_dev, mid, right))
        for k in range(kcount):
            line = jnp.broadcast_to(ext[k : k + 1], (rows, wide))
            turned = pltpu.roll(line, wide - reach - MAXLAG, 1, stride=1, stride_axis=0)
            win[step, k * rows : (k + 1) * rows, :] = turned[:, :lanes].astype(jnp.bfloat16)
        return carry

    def source_body(step, carry):
        @pl.when(step > 0)
        def _():
            field_copy(step).wait()

        got = recv[step]
        add_products(step, 0, count)
        add_sums(got)
        return carry

    count = kcount * rows

    def add_products(step, begin, end):
        acc[begin:end, :] += jnp.dot(
            win[step, begin:end, :t_dev], recv[step], preferred_element_type=jnp.float32
        )

    def add_sums(got):
        value = got.astype(jnp.float32)
        acc[kcount * rows : kcount * rows + 1, :] += jnp.sum(value, 0, keepdims=True)
        acc[kcount * rows + 1 : kcount * rows + 2, :] += jnp.sum(value * value, 0, keepdims=True)

    lax.fori_loop(0, chips, window_body, 0)
    lax.fori_loop(0, chips - 1, source_body, 0)

    def swap(place, begin, end):
        return pltpu.make_async_remote_copy(
            src_ref=acc.at[pl.ds(begin, end - begin)],
            dst_ref=acc_in.at[pl.ds(begin, end - begin)],
            send_sem=last_send.at[place],
            recv_sem=last_recv.at[place],
            device_id=(partner,),
            device_id_type=MESH,
        )

    middle = kcount // 2 * rows
    field_copy(chips - 1).wait()
    add_sums(recv[chips - 1])
    swaps = [swap(1, count, count + 8), swap(2, 0, middle), swap(3, middle, count)]
    swaps[0].start()
    add_products(chips - 1, 0, middle)
    swaps[1].start()
    add_products(chips - 1, middle, count)
    swaps[2].start()
    swaps[0].wait()
    half = cells // 2

    def mine(begin, end):
        total = acc[begin:end, :] + acc_in[begin:end, :]
        return jnp.where(core == 0, total[:, :half], total[:, half:])

    mean_x = mine(count, count + 1) / total_days
    var_x = mine(count + 1, count + 2) / total_days - mean_x * mean_x
    inner = total_days * jnp.sqrt(var_x + 1e-06)
    mask = mask_ref[...].astype(jnp.float32)
    outer = jnp.sqrt(var + 1e-06)
    lag = lag_ref[...]
    row = lax.broadcasted_iota(jnp.int32, (rows, lag.shape[1]), 0)
    for k in range(kcount):
        if k == 0:
            swaps[1].wait()
        if k == kcount // 2:
            swaps[2].wait()
        numer = mine(k * rows, (k + 1) * rows) - mean_x * totals[0:rows, k : k + 1]
        value = numer / (inner * outer[k : k + 1]) * mask
        chosen = jnp.where(row == lag + (offset_ref[k] + MAXLAG), 1.0, 0.0)
        out_ref[k] = lax.dot_general(
            value,
            chosen,
            (((0,), (0,)), ((), ())),
            precision=lax.Precision.HIGHEST,
            preferred_element_type=jnp.float32,
        )


def shards(field, index, lag_list, index_offset, sea_mask):
    t_dev, cells_all = field.shape
    devices = lax.axis_size("tm")
    kcount = index.shape[1]
    kpad = kcount
    lanes = round_up(t_dev, 128)
    rows = round_up(PLACES, 16)
    chips = devices // 2
    cells = cells_all // chips
    low = 1
    while low * low < chips:
        low *= 2
    high = chips // low
    sizes = (devices, t_dev, kcount, kpad, rows, low)
    dma = pltpu.SemaphoreType.DMA
    f32 = jnp.float32
    held = 4 * cells_all * t_dev + 4 * devices * round_up(kcount, 8) * lanes
    held += 2 * chips * kcount * rows * lanes + 8 * (kcount * rows + 8) * cells
    limit = held + 4 * 1024 * 1024
    vmem = pl.BlockSpec(memory_space=pltpu.VMEM)
    maps = pl.pallas_call(
        functools.partial(kernel, sizes),
        out_shape=jax.ShapeDtypeStruct((kcount, cells // 2, lag_list.shape[0]), f32),
        in_specs=[
            pl.BlockSpec(memory_space=pl.ANY),
            vmem,
            vmem,
            pl.BlockSpec(memory_space=pltpu.SMEM),
            vmem,
        ],
        out_specs=vmem,
        scratch_shapes=[
            pltpu.VMEM((t_dev, cells_all), jnp.bfloat16),
            pltpu.VMEM((kpad, lanes), f32),
            pltpu.VMEM((chips, t_dev, cells), jnp.bfloat16),
            pltpu.VMEM((devices, kpad, lanes), f32),
            pltpu.VMEM((chips, kcount * rows, lanes), jnp.bfloat16),
            pltpu.VMEM((kcount * rows + 8, cells), f32),
            pltpu.VMEM((kcount * rows + 8, cells), f32),
            dma((chips,)),
            dma((chips,)),
            dma((high,)),
            dma((high,)),
            dma((low,)),
            dma((low,)),
            dma((4,)),
            dma((4,)),
            dma((3,)),
        ],
        compiler_params=pltpu.CompilerParams(
            collective_id=0, has_side_effects=True, vmem_limit_bytes=60 * 1024 * 1024
        ),
    )(field, index.T, lag_list[None, :], index_offset, sea_mask[None, :])
    return jnp.transpose(maps, (1, 0, 2))


def solution(mesh):
    return jax.shard_map(
        shards,
        mesh=mesh,
        in_specs=(P("tm", None), P("tm", None), P(), P(), P("tm")),
        out_specs=P("tm", None, None),
        check_vma=False,
    )
```
